32 devices in a mesh: dp: 2 (over z, core), tp: 16 (over x, y).
Axes of the slice: x: 4, y: 4, z: 1, core: 2. Of those that a mesh axis runs over, the one named last changes fastest.
The devices are a block of a 4x4x8 slice.
Arguments:
- x: bfloat16 [128, 3072], P('dp'), parts along dimension 0
- k_cache: bfloat16 [128, 2048, 16, 256], P('dp', None, 'tp'), parts along dimension 0
- v_cache: bfloat16 [128, 2048, 16, 256], P('dp', None, 'tp'), parts along dimension 0
- gain_a: bfloat16 [3072], replicated
- wq: bfloat16 [3072, 4096], P(None, 'tp')
- wo: bfloat16 [4096, 3072], P('tp')
- gain_m: bfloat16 [3072], replicated
- w_gate: bfloat16 [3072, 24576], P(None, 'tp')
- w_up: bfloat16 [3072, 24576], P(None, 'tp')
- w_down: bfloat16 [24576, 3072], P('tp')
Outputs:
- output: bfloat16 [128, 3072], P('dp'), parts along dimension 0
There are 2 independent parts. The reference program is written for one: setup_inputs(seed, part) draws one part's arguments, and reference() takes and returns one part's arrays. A program takes and returns all parts, laid end to end along the dimension named above; an argument that names none is the same for every part.
All inputs are finite; a program needn't handle non-finite values.
Results may differ from the reference program's by a relative error of at most 0.017.
Values are sent between devices in bfloat16 or wider.
A program may use at most 768 MiB of HBM per device.

```python
import jax
import jax.numpy as jnp
from jax import lax

BATCH = 64
CACHE = 2048
D = 3072
HEADS = 16
KV_HEADS = 16
HEAD = 256
FF = 24576
THETA = 10000


def setup_inputs(seed: int = 0, part: int = 0) -> dict:
    kx, kc, kw, kn, kq, ko, km, kg, ku, kd = jax.random.split(jax.random.key(seed), 10)
    kx, kc, kw = (jax.random.fold_in(k, part) for k in (kx, kc, kw))

    def weights(key, rows, columns):
        return jax.random.normal(key, (rows, columns), jnp.float32) * rows**-0.5

    drawn = {
        "x": jax.random.normal(kx, (BATCH, D), jnp.float32),
        "k_cache": 2 * jax.random.normal(kc, (BATCH, CACHE, KV_HEADS, HEAD), jnp.float32),
        "v_cache": 4 * jax.random.normal(kw, (BATCH, CACHE, KV_HEADS, HEAD), jnp.float32),
        "gain_a": 1 + 0.1 * jax.random.normal(kn, (D,), jnp.float32),
        "wq": 2 * weights(kq, D, HEADS * HEAD),
        "wo": weights(ko, HEADS * HEAD, D),
        "gain_m": 1 + 0.1 * jax.random.normal(km, (D,), jnp.float32),
        "w_gate": weights(kg, D, FF),
        "w_up": weights(ku, D, FF),
        "w_down": 2 * weights(kd, FF, D),
    }
    return {k: v.astype(jnp.bfloat16) for k, v in drawn.items()}


def normed(x, gain):
    wide = x.astype(jnp.float32)
    scale = lax.rsqrt(jnp.mean(wide * wide, -1, keepdims=True) + 1e-6)
    return (wide * scale * gain.astype(jnp.float32)).astype(jnp.bfloat16)


def turned(t, place, theta):
    half = t.shape[-1] // 2
    angle = place.astype(jnp.float32)[:, None] * theta ** (-jnp.arange(half, dtype=jnp.float32) / half)
    cos, sin = jnp.cos(angle)[:, None], jnp.sin(angle)[:, None]
    a, b = t[..., :half].astype(jnp.float32), t[..., half:].astype(jnp.float32)
    return jnp.concatenate([a * cos - b * sin, b * cos + a * sin], -1).astype(jnp.bfloat16)


def matmul(a, w):
    return jnp.dot(a, w, preferred_element_type=jnp.float32).astype(jnp.bfloat16)


def einsum(form, a, b):
    return jnp.einsum(form, a.astype(jnp.float32), b.astype(jnp.float32))


def seen_by(a, wq, k_cache, v_cache, head, theta):
    batch, cache, kv_heads = k_cache.shape[:3]
    place = jnp.full((batch,), cache - 1)
    q = turned(matmul(a, wq).reshape(batch, -1, head), place, theta).reshape(batch, kv_heads, -1, head)
    scores = einsum("bgsd,bugd->bgsu", q, k_cache) * head**-0.5
    weights = jax.nn.softmax(scores, -1).astype(jnp.bfloat16)
    return einsum("bgsu,bugd->bgsd", weights, v_cache).astype(jnp.bfloat16).reshape(batch, -1)


def hidden_of(b, w_gate, w_up):
    gate = jnp.dot(b, w_gate, preferred_element_type=jnp.float32)
    up = jnp.dot(b, w_up, preferred_element_type=jnp.float32)
    return (jax.nn.silu(gate) * up).astype(jnp.bfloat16)


def reference(x, k_cache, v_cache, gain_a, wq, wo, gain_m, w_gate, w_up, w_down):
    seen = seen_by(normed(x, gain_a), wq, k_cache, v_cache, HEAD, THETA)
    h = (x.astype(jnp.float32) + jnp.dot(seen, wo, preferred_element_type=jnp.float32)).astype(jnp.bfloat16)
    hidden = hidden_of(normed(h, gain_m), w_gate, w_up)
    return (h.astype(jnp.float32) + jnp.dot(hidden, w_down, preferred_element_type=jnp.float32)).astype(jnp.bfloat16)
```

```python
import functools

import jax
import jax.numpy as jnp
import numpy as np
from jax import lax
from jax.experimental import pallas as pl
from jax.experimental.pallas import tpu as pltpu
from jax.sharding import PartitionSpec as P

THETA = 10000
EPS = 1e-6
GROUP = 8
PIECE = 4
CHUNK = 16
SUB = 8
MESH = pl.DeviceIdType.MESH
BF16, F32 = jnp.bfloat16, jnp.float32


def normed(wide, gain):
    scale = lax.rsqrt(jnp.mean(wide * wide, -1, keepdims=True) + EPS)
    return (wide * scale * gain).astype(BF16)


def dot(a, b):
    return jnp.dot(a, b, preferred_element_type=F32)


def kernel(n, x_hbm, k_hbm, v_hbm, ga_hbm, wq_hbm, wo_hbm, gm_hbm, wg_hbm, wu_hbm, wd_hbm, trig_hbm, out_ref,
           x_v, ga_v, gm_v, trig_v, wq_v, wo_v, wg_v, wu_v, wd_v, ring, x32, h32, q32, seen32, act, hidden,
           own1, term1, rs1, hb, own2, term2, rs2, yb,
           in_sem, w_sem, ring_sem, send1, recv1, send2, recv2, send3, recv3, send4, recv4):
    me = lax.axis_index("tp")
    rows, d = x_v.shape
    head = q32.shape[1]
    half = head // 2
    groups = rows // GROUP
    chunks = rows // CHUNK
    cols1 = d * CHUNK // (n * SUB)
    per_row1 = d // cols1
    width2 = d // chunks
    per_row2 = width2 // cols1

    def fetch(src, dst, sem):
        return pltpu.make_async_copy(src, dst, sem)

    small = [
        fetch(x_hbm, x_v, in_sem.at[0]),
        fetch(ga_hbm, ga_v, in_sem.at[1]),
        fetch(wq_hbm, wq_v, in_sem.at[2]),
        fetch(trig_hbm, trig_v, in_sem.at[3]),
        fetch(wo_hbm, wo_v, in_sem.at[4]),
        fetch(gm_hbm, gm_v, in_sem.at[5]),
    ]
    weights = [fetch(wg_hbm, wg_v, w_sem.at[0]), fetch(wu_hbm, wu_v, w_sem.at[1]), fetch(wd_hbm, wd_v, w_sem.at[2])]

    def piece(g, j):
        src = k_hbm if j < 2 else v_hbm
        return fetch(src.at[pl.ds(g * GROUP + (j % 2) * PIECE, PIECE)], ring.at[j], ring_sem.at[j])

    for c in small[:4]:
        c.start()
    for j in range(4):
        piece(0, j).start()
    for c in small[4:]:
        c.start()

    barrier = pltpu.get_barrier_semaphore()
    for r in range(1, n):
        pl.semaphore_signal(barrier, inc=1, device_id={"tp": lax.rem(me + r, n)}, device_id_type=MESH)

    small[0].wait()
    small[1].wait()
    wide = x_v[...].astype(F32)
    x32[...] = wide
    act[...] = normed(wide, ga_v[...].astype(F32))
    small[2].wait()
    small[3].wait()
    q = dot(act[...], wq_v[...]).astype(BF16).astype(F32)
    cos, sin = trig_v[0:1, :], trig_v[1:2, :]
    a, b = q[:, :half], q[:, half:]
    q32[:, :half] = (a * cos - b * sin).astype(BF16).astype(F32)
    q32[:, half:] = (b * cos + a * sin).astype(BF16).astype(F32)
    small[4].wait()
    small[5].wait()
    pl.semaphore_wait(barrier, n - 1)

    def total(buf, sem):
        fetch(buf.at[pl.ds(0, n - 1)], buf.at[pl.ds(0, n - 1)], sem).wait()

    def scatter(term, land, send, recv):
        for r in range(1, n):
            to = lax.rem(me + r, n)
            pltpu.make_async_remote_copy(
                src_ref=term.at[to], dst_ref=land.at[r - 1], send_sem=send, recv_sem=recv, device_id={"tp": to}, device_id_type=MESH
            ).start()

    def gather(buf, send, recv):
        for r in range(1, n):
            to = lax.rem(me + r, n)
            pltpu.make_async_remote_copy(
                src_ref=buf.at[me], dst_ref=buf.at[me], send_sem=send, recv_sem=recv, device_id={"tp": to}, device_id_type=MESH
            ).start()

    def summed(own, land):
        s = own[me]
        for r in range(n - 1):
            s = s + land[r].astype(F32)
        return s

    def send_first(c):
        res = dot(seen32[pl.ds(pl.multiple_of(c * CHUNK, CHUNK), CHUNK), :].astype(BF16), wo_v[...])
        for s in range(n):
            rg, cg = divmod(s, per_row1)
            part = res[rg * SUB : (rg + 1) * SUB, cg * cols1 : (cg + 1) * cols1]
            own1[s] = part
            term1[c, s] = part.astype(BF16)
        scatter(term1.at[c], rs1.at[c], send1.at[c], recv1.at[c])

    def sum_first(c):
        total(rs1.at[c], recv1.at[c])
        s = summed(own1, rs1.at[c])
        row = pl.multiple_of(c * CHUNK + me // per_row1 * SUB, SUB)
        col = pl.multiple_of(lax.rem(me, per_row1) * cols1, 128)
        hb[c, me] = (x32[pl.ds(row, SUB), pl.ds(col, cols1)] + s).astype(BF16)
        gather(hb.at[c], send2.at[c], recv2.at[c])

    row_of = lax.broadcasted_iota(jnp.int32, (GROUP, 1), 0)

    def group(g, carry):
        def refill(j):
            @pl.when(g < groups - 1)
            def _():
                piece(g + 1, j).start()

            if j < 3:
                @pl.when(g == groups - 1)
                def _():
                    weights[j].start()

        qg = q32[pl.ds(pl.multiple_of(g * GROUP, GROUP), GROUP), :]
        s = None
        for j in range(2):
            piece(g, j).wait()
            for i in range(PIECE):
                qm = jnp.where(row_of == j * PIECE + i, qg, 0.0).astype(BF16)
                t = lax.dot_general(qm, ring[j, i], (((1,), (1,)), ((), ())), preferred_element_type=F32)
                s = t if s is None else s + t
            refill(j)
        s = s * head**-0.5
        p = jnp.exp(s - jnp.max(s, -1, keepdims=True))
        w = p / jnp.sum(p, -1, keepdims=True)
        o = None
        for j in range(2, 4):
            piece(g, j).wait()
            for i in range(PIECE):
                wm = jnp.where(row_of == (j - 2) * PIECE + i, w, 0.0).astype(BF16)
                t = dot(wm, ring[j, i])
                o = t if o is None else o + t
            refill(j)
        seen32[pl.ds(pl.multiple_of(g * GROUP, GROUP), GROUP), :] = o
        per = CHUNK // GROUP

        @pl.when(lax.rem(g, per) == per - 1)
        def _():
            send_first(g // per)

        @pl.when(jnp.logical_and(lax.rem(g, per) == 0, g > 0))
        def _():
            sum_first(g // per - 1)

        return carry

    lax.fori_loop(0, groups, group, 0)
    sum_first(chunks - 1)

    gm = gm_v[...].astype(F32)
    for c in range(chunks):
        total(hb.at[c], recv2.at[c])
        h = jnp.concatenate(
            [
                jnp.concatenate([hb[c, rg * per_row1 + cg].astype(F32) for cg in range(per_row1)], 1)
                for rg in range(CHUNK // SUB)
            ],
            0,
        )
        h32[c * CHUNK : (c + 1) * CHUNK, :] = h
        act[c * CHUNK : (c + 1) * CHUNK, :] = normed(h, gm)

    weights[0].wait()
    weights[1].wait()
    block = 256

    def up(i, carry):
        at = pl.ds(pl.multiple_of(i * block, block), block)
        gate = dot(act[...], wg_v[:, at])
        hidden[:, at] = (jax.nn.silu(gate) * dot(act[...], wu_v[:, at])).astype(BF16)
        return carry

    lax.fori_loop(0, wg_v.shape[1] // block, up, 0)
    weights[2].wait()

    for c in range(chunks):
        res = dot(hidden[...], wd_v[:, c * width2 : (c + 1) * width2])
        for s in range(n):
            rg, cg = divmod(s, per_row2)
            part = res[rg * SUB : (rg + 1) * SUB, cg * cols1 : (cg + 1) * cols1]
            own2[c, s] = part
            term2[c, s] = part.astype(BF16)
        scatter(term2.at[c], rs2.at[c], send3.at[c], recv3.at[c])

    for c in range(chunks):
        total(rs2.at[c], recv3.at[c])
        s = summed(own2.at[c], rs2.at[c])
        row = pl.multiple_of(me // per_row2 * SUB, SUB)
        col = pl.multiple_of(c * width2 + lax.rem(me, per_row2) * cols1, 128)
        yb[c, me] = (h32[pl.ds(row, SUB), pl.ds(col, cols1)] + s).astype(BF16)
        gather(yb.at[c], send4.at[c], recv4.at[c])

    for c in range(chunks):
        total(yb.at[c], recv4.at[c])
        for rg in range(0, rows // SUB, 2):
            for cg in range(per_row2):
                pair = [yb[c, (rg + k) * per_row2 + cg].astype(F32) for k in range(2)]
                col = c * width2 + cg * cols1
                out_ref[rg * SUB : (rg + 2) * SUB, col : col + cols1] = jnp.concatenate(pair, 0).astype(BF16)

    for c in range(chunks):
        total(term1.at[c], send1.at[c])
        total(hb.at[c], send2.at[c])
        total(term2.at[c], send3.at[c])
        total(yb.at[c], send4.at[c])


def solution(mesh):
    n = mesh.shape["tp"]

    def step(x, k_cache, v_cache, gain_a, wq, wo, gain_m, w_gate, w_up, w_down):
        rows, d = x.shape
        cache = k_cache.shape[1]
        head = k_cache.shape[3]
        ff = w_gate.shape[1]
        half = head // 2
        angle = (cache - 1) * float(THETA) ** (-np.arange(half, dtype=np.float64) / half)
        trig = jnp.asarray(np.stack([np.cos(angle), np.sin(angle)]).astype(np.float32))
        chunks = rows // CHUNK
        share = (SUB, rows * d // chunks // n // SUB)
        any_spec = pl.BlockSpec(memory_space=pl.ANY)
        dma = pltpu.SemaphoreType.DMA
        call = pl.pallas_call(
            functools.partial(kernel, n),
            out_shape=jax.ShapeDtypeStruct((rows, d), BF16),
            in_specs=[any_spec] * 11,
            out_specs=pl.BlockSpec(memory_space=pltpu.VMEM),
            scratch_shapes=[
                pltpu.VMEM((rows, d), BF16),
                pltpu.VMEM((1, d), BF16),
                pltpu.VMEM((1, d), BF16),
                pltpu.VMEM((2, half), F32),
                pltpu.VMEM((d, head), BF16),
                pltpu.VMEM((head, d), BF16),
                pltpu.VMEM((d, ff), BF16),
                pltpu.VMEM((d, ff), BF16),
                pltpu.VMEM((ff, d), BF16),
                pltpu.VMEM((4, PIECE, cache, head), BF16),
                pltpu.VMEM((rows, d), F32),
                pltpu.VMEM((rows, d), F32),
                pltpu.VMEM((rows, head), F32),
                pltpu.VMEM((rows, head), F32),
                pltpu.VMEM((rows, d), BF16),
                pltpu.VMEM((rows, ff), BF16),
                pltpu.VMEM((n, *share), F32),
                pltpu.VMEM((chunks, n, *share), BF16),
                pltpu.VMEM((chunks, n - 1, *share), BF16),
                pltpu.VMEM((chunks, n, *share), BF16),
                pltpu.VMEM((chunks, n, *share), F32),
                pltpu.VMEM((chunks, n, *share), BF16),
                pltpu.VMEM((chunks, n - 1, *share), BF16),
                pltpu.VMEM((chunks, n, *share), BF16),
                dma((6,)),
                dma((3,)),
                dma((4,)),
            ]
            + [dma((chunks,))] * 8,
            compiler_params=pltpu.CompilerParams(collective_id=0, has_side_effects=True, vmem_limit_bytes=63 * 2**20),
        )
        flat = (rows, cache, head)
        return call(
            x, k_cache.reshape(flat), v_cache.reshape(flat), gain_a.reshape(1, d), wq, wo, gain_m.reshape(1, d), w_gate, w_up, w_down, trig
        )

    states, cache, columns, rows_of = P("dp", None), P("dp", None, "tp", None), P(None, "tp"), P("tp", None)
    return jax.shard_map(
        step,
        mesh=mesh,
        in_specs=(states, cache, cache, P(None), columns, rows_of, P(None), columns, columns, rows_of),
        out_specs=states,
        check_vma=False,
    )
```

```python
import functools

import jax
import jax.numpy as jnp
import numpy as np
from jax import lax
from jax.experimental import pallas as pl
from jax.experimental.pallas import tpu as pltpu
from jax.sharding import PartitionSpec as P

THETA = 10000
EPS = 1e-6
GROUP = 16
PIECE = 4
CHUNK = 16
SUB = 8
MESH = pl.DeviceIdType.MESH
BF16, F32 = jnp.bfloat16, jnp.float32


def normed(wide, gain):
    scale = lax.rsqrt(jnp.mean(wide * wide, -1, keepdims=True) + EPS)
    return (wide * scale * gain).astype(BF16)


def dot(a, b):
    return jnp.dot(a, b, preferred_element_type=F32)


def kernel(n, x_hbm, k_hbm, v_hbm, ga_hbm, wq_hbm, wo_hbm, gm_hbm, wg_hbm, wu_hbm, wd_hbm, trig_hbm, out_ref,
           x_v, ga_v, gm_v, trig_v, wq_v, wo_v, wg_v, wu_v, wd_v, ring, x32, h32, q32, seen32, scores, act, hidden,
           own1, term1, rs1, hb, own2, term2, rs2, yb,
           in_sem, w_sem, ring_sem, send1, recv1, send2, recv2, send3, recv3, send4, recv4):
    me = lax.axis_index("tp")
    rows, d = x_v.shape
    head = q32.shape[1]
    half = head // 2
    groups = rows // GROUP
    chunks = rows // CHUNK
    cols1 = d * CHUNK // (n * SUB)
    per_row1 = d // cols1
    width2 = d // chunks
    per_row2 = width2 // cols1

    def fetch(src, dst, sem):
        return pltpu.make_async_copy(src, dst, sem)

    small = [
        fetch(x_hbm, x_v, in_sem.at[0]),
        fetch(ga_hbm, ga_v, in_sem.at[1]),
        fetch(wq_hbm, wq_v, in_sem.at[2]),
        fetch(trig_hbm, trig_v, in_sem.at[3]),
        fetch(wo_hbm, wo_v, in_sem.at[4]),
        fetch(gm_hbm, gm_v, in_sem.at[5]),
    ]
    weights = [fetch(wg_hbm, wg_v, w_sem.at[0]), fetch(wu_hbm, wu_v, w_sem.at[1]), fetch(wd_hbm, wd_v, w_sem.at[2])]

    def piece(src, g, j):
        return fetch(src.at[pl.ds(g * GROUP + j * PIECE, PIECE)], ring.at[j], ring_sem.at[j])

    for c in small[:4]:
        c.start()
    for j in range(GROUP // PIECE):
        piece(k_hbm, 0, j).start()
    for c in small[4:]:
        c.start()

    barrier = pltpu.get_barrier_semaphore()
    for r in range(1, n):
        pl.semaphore_signal(barrier, inc=1, device_id={"tp": lax.rem(me + r, n)}, device_id_type=MESH)

    small[0].wait()
    small[1].wait()
    wide = x_v[...].astype(F32)
    x32[...] = wide
    act[...] = normed(wide, ga_v[...].astype(F32))
    small[2].wait()
    small[3].wait()
    q = dot(act[...], wq_v[...]).astype(BF16).astype(F32)
    cos, sin = trig_v[0:1, :], trig_v[1:2, :]
    a, b = q[:, :half], q[:, half:]
    q32[:, :half] = (a * cos - b * sin).astype(BF16).astype(F32)
    q32[:, half:] = (b * cos + a * sin).astype(BF16).astype(F32)
    small[4].wait()
    small[5].wait()
    pl.semaphore_wait(barrier, n - 1)

    def total(buf, sem):
        fetch(buf.at[pl.ds(0, n - 1)], buf.at[pl.ds(0, n - 1)], sem).wait()

    def scatter(term, land, send, recv):
        for r in range(1, n):
            to = lax.rem(me + r, n)
            pltpu.make_async_remote_copy(
                src_ref=term.at[to], dst_ref=land.at[r - 1], send_sem=send, recv_sem=recv, device_id={"tp": to}, device_id_type=MESH
            ).start()

    def gather(buf, send, recv):
        for r in range(1, n):
            to = lax.rem(me + r, n)
            pltpu.make_async_remote_copy(
                src_ref=buf.at[me], dst_ref=buf.at[me], send_sem=send, recv_sem=recv, device_id={"tp": to}, device_id_type=MESH
            ).start()

    def summed(own, land):
        s = own[me]
        for r in range(n - 1):
            s = s + land[r].astype(F32)
        return s

    def send_first(c):
        res = dot(seen32[pl.ds(pl.multiple_of(c * CHUNK, CHUNK), CHUNK), :].astype(BF16), wo_v[...])
        for s in range(n):
            rg, cg = divmod(s, per_row1)
            part = res[rg * SUB : (rg + 1) * SUB, cg * cols1 : (cg + 1) * cols1]
            own1[s] = part
            term1[c, s] = part.astype(BF16)
        scatter(term1.at[c], rs1.at[c], send1.at[c], recv1.at[c])

    def sum_first(c):
        total(rs1.at[c], recv1.at[c])
        s = summed(own1, rs1.at[c])
        row = pl.multiple_of(c * CHUNK + me // per_row1 * SUB, SUB)
        col = pl.multiple_of(lax.rem(me, per_row1) * cols1, 128)
        hb[c, me] = (x32[pl.ds(row, SUB), pl.ds(col, cols1)] + s).astype(BF16)
        gather(hb.at[c], send2.at[c], recv2.at[c])

    row_of = lax.broadcasted_iota(jnp.int32, (GROUP, 1), 0)
    pieces = GROUP // PIECE

    def group(g, carry):
        at = pl.ds(pl.multiple_of(g * GROUP, GROUP), GROUP)

        def scores_of(j, carry):
            qg = q32[at, :]
            piece(k_hbm, g, j).wait()
            s = None
            for i in range(PIECE):
                qm = jnp.where(row_of == j * PIECE + i, qg, 0.0).astype(BF16)
                t = lax.dot_general(qm, ring[j, i], (((1,), (1,)), ((), ())), preferred_element_type=F32)
                s = t if s is None else s + t
            scores[...] = jnp.where(row_of // PIECE == j, s, scores[...])
            piece(v_hbm, g, j).start()
            return carry

        def seen_of(j, carry):
            piece(v_hbm, g, j).wait()
            o = []
            for i in range(PIECE):
                wm = jnp.where(row_of == j * PIECE + i, scores[...], 0.0).astype(BF16)
                o.append(dot(wm, ring[j, i]))
            o = jnp.where(row_of < j * PIECE + PIECE // 2, sum(o[1 : PIECE // 2], o[0]), sum(o[PIECE // 2 + 1 :], o[PIECE // 2]))
            seen32[at, :] = jnp.where(row_of // PIECE == j, o, seen32[at, :])

            @pl.when(g < groups - 1)
            def _():
                piece(k_hbm, g + 1, j).start()

            for w in range(3):
                @pl.when(jnp.logical_and(g == groups - 1, j == w))
                def _():
                    weights[w].start()

            return carry

        lax.fori_loop(0, pieces, scores_of, 0)
        s = scores[...] * head**-0.5
        p = jnp.exp(s - jnp.max(s, -1, keepdims=True))
        scores[...] = p / jnp.sum(p, -1, keepdims=True)
        lax.fori_loop(0, pieces, seen_of, 0)

        @pl.when(g > 0)
        def _():
            sum_first(g - 1)

        send_first(g)
        return carry

    lax.fori_loop(0, groups, group, 0)
    sum_first(chunks - 1)

    gm = gm_v[...].astype(F32)
    for c in range(chunks):
        total(hb.at[c], recv2.at[c])
        h = jnp.concatenate(
            [
                jnp.concatenate([hb[c, rg * per_row1 + cg].astype(F32) for cg in range(per_row1)], 1)
                for rg in range(CHUNK // SUB)
            ],
            0,
        )
        h32[c * CHUNK : (c + 1) * CHUNK, :] = h
        act[c * CHUNK : (c + 1) * CHUNK, :] = normed(h, gm)

    weights[0].wait()
    weights[1].wait()
    block = 256

    def up(i, carry):
        at = pl.ds(pl.multiple_of(i * block, block), block)
        gate = dot(act[...], wg_v[:, at])
        hidden[:, at] = (jax.nn.silu(gate) * dot(act[...], wu_v[:, at])).astype(BF16)
        return carry

    lax.fori_loop(0, wg_v.shape[1] // block, up, 0)
    weights[2].wait()

    for c in range(chunks):
        res = dot(hidden[...], wd_v[:, c * width2 : (c + 1) * width2])
        for s in range(n):
            rg, cg = divmod(s, per_row2)
            part = res[rg * SUB : (rg + 1) * SUB, cg * cols1 : (cg + 1) * cols1]
            own2[c, s] = part
            term2[c, s] = part.astype(BF16)
        scatter(term2.at[c], rs2.at[c], send3.at[c], recv3.at[c])

    for c in range(chunks):
        total(rs2.at[c], recv3.at[c])
        s = summed(own2.at[c], rs2.at[c])
        row = pl.multiple_of(me // per_row2 * SUB, SUB)
        col = pl.multiple_of(c * width2 + lax.rem(me, per_row2) * cols1, 128)
        yb[c, me] = (h32[pl.ds(row, SUB), pl.ds(col, cols1)] + s).astype(BF16)
        gather(yb.at[c], send4.at[c], recv4.at[c])

    for c in range(chunks):
        total(yb.at[c], recv4.at[c])
        for rg in range(0, rows // SUB, 2):
            for cg in range(per_row2):
                pair = [yb[c, (rg + k) * per_row2 + cg].astype(F32) for k in range(2)]
                col = c * width2 + cg * cols1
                out_ref[rg * SUB : (rg + 2) * SUB, col : col + cols1] = jnp.concatenate(pair, 0).astype(BF16)

    for c in range(chunks):
        total(term1.at[c], send1.at[c])
        total(hb.at[c], send2.at[c])
        total(term2.at[c], send3.at[c])
        total(yb.at[c], send4.at[c])


def solution(mesh):
    n = mesh.shape["tp"]

    def step(x, k_cache, v_cache, gain_a, wq, wo, gain_m, w_gate, w_up, w_down):
        rows, d = x.shape
        cache = k_cache.shape[1]
        head = k_cache.shape[3]
        ff = w_gate.shape[1]
        half = head // 2
        angle = (cache - 1) * float(THETA) ** (-np.arange(half, dtype=np.float64) / half)
        trig = jnp.asarray(np.stack([np.cos(angle), np.sin(angle)]).astype(np.float32))
        chunks = rows // CHUNK
        share = (SUB, rows * d // chunks // n // SUB)
        any_spec = pl.BlockSpec(memory_space=pl.ANY)
        dma = pltpu.SemaphoreType.DMA
        call = pl.pallas_call(
            functools.partial(kernel, n),
            out_shape=jax.ShapeDtypeStruct((rows, d), BF16),
            in_specs=[any_spec] * 11,
            out_specs=pl.BlockSpec(memory_space=pltpu.VMEM),
            scratch_shapes=[
                pltpu.VMEM((rows, d), BF16),
                pltpu.VMEM((1, d), BF16),
                pltpu.VMEM((1, d), BF16),
                pltpu.VMEM((2, half), F32),
                pltpu.VMEM((d, head), BF16),
                pltpu.VMEM((head, d), BF16),
                pltpu.VMEM((d, ff), BF16),
                pltpu.VMEM((d, ff), BF16),
                pltpu.VMEM((ff, d), BF16),
                pltpu.VMEM((GROUP // PIECE, PIECE, cache, head), BF16),
                pltpu.VMEM((rows, d), F32),
                pltpu.VMEM((rows, d), F32),
                pltpu.VMEM((rows, head), F32),
                pltpu.VMEM((rows, head), F32),
                pltpu.VMEM((GROUP, cache), F32),
                pltpu.VMEM((rows, d), BF16),
                pltpu.VMEM((rows, ff), BF16),
                pltpu.VMEM((n, *share), F32),
                pltpu.VMEM((chunks, n, *share), BF16),
                pltpu.VMEM((chunks, n - 1, *share), BF16),
                pltpu.VMEM((chunks, n, *share), BF16),
                pltpu.VMEM((chunks, n, *share), F32),
                pltpu.VMEM((chunks, n, *share), BF16),
                pltpu.VMEM((chunks, n - 1, *share), BF16),
                pltpu.VMEM((chunks, n, *share), BF16),
                dma((6,)),
                dma((3,)),
                dma((GROUP // PIECE,)),
            ]
            + [dma((chunks,))] * 8,
            compiler_params=pltpu.CompilerParams(collective_id=0, has_side_effects=True, vmem_limit_bytes=63 * 2**20),
        )
        flat = (rows, cache, head)
        return call(
            x, k_cache.reshape(flat), v_cache.reshape(flat), gain_a.reshape(1, d), wq, wo, gain_m.reshape(1, d), w_gate, w_up, w_down, trig
        )

    states, cache, columns, rows_of = P("dp", None), P("dp", None, "tp", None), P(None, "tp"), P("tp", None)
    return jax.shard_map(
        step,
        mesh=mesh,
        in_specs=(states, cache, cache, P(None), columns, rows_of, P(None), columns, columns, rows_of),
        out_specs=states,
        check_vma=False,
    )
```

```python
import functools

import jax
import jax.numpy as jnp
import numpy as np
from jax import lax
from jax.experimental import pallas as pl
from jax.experimental.pallas import tpu as pltpu
from jax.sharding import PartitionSpec as P

THETA = 10000
EPS = 1e-6
GROUP = 16
PIECE = 4
CHUNK = 16
SUB = 8
MESH = pl.DeviceIdType.MESH
BF16, F32 = jnp.bfloat16, jnp.float32


def normed(wide, gain):
    scale = lax.rsqrt(jnp.mean(wide * wide, -1, keepdims=True) + EPS)
    return (wide * scale * gain).astype(BF16)


def dot(a, b):
    return jnp.dot(a, b, preferred_element_type=F32)


def kernel(n, x_hbm, k_hbm, v_hbm, ga_hbm, wq_hbm, wo_hbm, gm_hbm, wg_hbm, wu_hbm, wd_hbm, trig_hbm, out_ref,
           x_v, ga_v, gm_v, trig_v, wq_v, wo_v, wg_v, wu_v, wd_v, ring, x32, h32, q32, seen32, scores, act, hidden,
           gates, own1, term1, rs1, hb, own2, term2, rs2, yb, own3, term3, rs3, yc,
           in_sem, w_sem, ring_sem, send1, recv1, send2, recv2, send3, recv3, send4, recv4):
    me = lax.axis_index("tp")
    rows, d = x_v.shape
    head = q32.shape[1]
    half = head // 2
    groups = rows // GROUP
    chunks = rows // CHUNK
    across = n * SUB // CHUNK
    wide1 = d // across

    def fetch(src, dst, sem):
        return pltpu.make_async_copy(src, dst, sem)

    small = [
        fetch(x_hbm, x_v, in_sem.at[0]),
        fetch(ga_hbm, ga_v, in_sem.at[1]),
        fetch(wq_hbm, wq_v, in_sem.at[2]),
        fetch(trig_hbm, trig_v, in_sem.at[3]),
        fetch(wo_hbm, wo_v, in_sem.at[4]),
        fetch(gm_hbm, gm_v, in_sem.at[5]),
    ]
    weights = [fetch(wg_hbm, wg_v, w_sem.at[0]), fetch(wu_hbm, wu_v, w_sem.at[1]), fetch(wd_hbm, wd_v, w_sem.at[2])]

    def piece(src, g, j):
        return fetch(src.at[pl.ds(g * GROUP + j * PIECE, PIECE)], ring.at[j], ring_sem.at[j])

    for c in small[:4]:
        c.start()
    for j in range(GROUP // PIECE):
        piece(k_hbm, 0, j).start()
    for c in small[4:]:
        c.start()

    barrier = pltpu.get_barrier_semaphore()
    for r in range(1, n):
        pl.semaphore_signal(barrier, inc=1, device_id={"tp": lax.rem(me + r, n)}, device_id_type=MESH)

    small[0].wait()
    small[1].wait()
    wide = x_v[...].astype(F32)
    x32[...] = wide
    act[...] = normed(wide, ga_v[...].astype(F32).reshape(1, d))
    small[2].wait()
    small[3].wait()
    q = dot(act[...], wq_v[...]).astype(BF16).astype(F32)
    cos, sin = trig_v[0:1, :], trig_v[1:2, :]
    a, b = q[:, :half], q[:, half:]
    q32[:, :half] = (a * cos - b * sin).astype(BF16).astype(F32)
    q32[:, half:] = (b * cos + a * sin).astype(BF16).astype(F32)
    small[4].wait()
    small[5].wait()
    pl.semaphore_wait(barrier, n - 1)

    def total(buf, sem):
        fetch(buf.at[pl.ds(0, n - 1)], buf.at[pl.ds(0, n - 1)], sem).wait()

    def send_to(to, src, dst, send, recv):
        pltpu.make_async_remote_copy(
            src_ref=src, dst_ref=dst, send_sem=send, recv_sem=recv, device_id={"tp": to}, device_id_type=MESH
        ).start()

    def gather(buf, send, recv):
        for r in range(1, n):
            send_to(lax.rem(me + r, n), buf.at[me], buf.at[me], send, recv)

    def share_of(states, row, buf):
        tall, wide = buf.shape[1:]
        row = pl.multiple_of(row + me // across * tall, SUB)
        return states[pl.ds(row, tall), pl.ds(pl.multiple_of(lax.rem(me, across) * wide, 128), wide)]

    def finish(states, row, own, land, buf, recv, send_next, recv_next):
        total(land, recv)
        s = own[me]
        for r in range(n - 1):
            s = s + land[r].astype(F32)
        buf[me] = (share_of(states, row, buf) + s).astype(BF16)
        gather(buf, send_next, recv_next)

    def whole(buf):
        rows_of = [jnp.concatenate([buf[rg * across + cg].astype(F32) for cg in range(across)], 1) for rg in range(n // across)]
        return jnp.concatenate(rows_of, 0)

    def send_first(c):
        res = dot(seen32[pl.ds(pl.multiple_of(c * CHUNK, CHUNK), CHUNK), :].astype(BF16), wo_v[...])
        for to in range(n):
            rg, cg = divmod(to, across)
            part = res[rg * SUB : (rg + 1) * SUB, cg * wide1 : (cg + 1) * wide1]
            own1[c, to] = part
            term1[c, to] = part.astype(BF16)
        for r in range(1, n):
            to = lax.rem(me + r, n)
            send_to(to, term1.at[c, to], rs1.at[c, r - 1], send1.at[c], recv1.at[c])

    def sum_first(c):
        finish(x32, c * CHUNK, own1.at[c], rs1.at[c], hb.at[c], recv1.at[c], send2.at[c], recv2.at[c])

    def norm_first(c):
        total(hb.at[c], recv2.at[c])
        h = whole(hb.at[c])
        at = pl.ds(pl.multiple_of(c * CHUNK, CHUNK), CHUNK)
        h32[at, :] = h
        act[at, :] = normed(h, gm_v[...].astype(F32).reshape(1, d))

    row_of = lax.broadcasted_iota(jnp.int32, (GROUP, 1), 0)
    pieces = GROUP // PIECE

    def group(g, carry):
        at = pl.ds(pl.multiple_of(g * GROUP, GROUP), GROUP)

        def scores_of(j, carry):
            qg = q32[at, :]
            piece(k_hbm, g, j).wait()
            s = None
            for i in range(PIECE):
                qm = jnp.where(row_of == j * PIECE + i, qg, 0.0).astype(BF16)
                t = lax.dot_general(qm, ring[j, i], (((1,), (1,)), ((), ())), preferred_element_type=F32)
                s = t if s is None else s + t
            scores[...] = jnp.where(row_of // PIECE == j, s, scores[...])
            piece(v_hbm, g, j).start()
            return carry

        def seen_of(j, carry):
            piece(v_hbm, g, j).wait()
            o = []
            for i in range(PIECE):
                wm = jnp.where(row_of == j * PIECE + i, scores[...], 0.0).astype(BF16)
                o.append(dot(wm, ring[j, i]))
            o = jnp.where(row_of < j * PIECE + PIECE // 2, sum(o[1 : PIECE // 2], o[0]), sum(o[PIECE // 2 + 1 :], o[PIECE // 2]))
            seen32[at, :] = jnp.where(row_of // PIECE == j, o, seen32[at, :])

            @pl.when(g < groups - 1)
            def _():
                piece(k_hbm, g + 1, j).start()

            for w in range(3):
                @pl.when(jnp.logical_and(g == groups - 1, j == w))
                def _():
                    weights[w].start()

            return carry

        lax.fori_loop(0, pieces, scores_of, 0)
        s = scores[...] * head**-0.5
        p = jnp.exp(s - jnp.max(s, -1, keepdims=True))
        scores[...] = p / jnp.sum(p, -1, keepdims=True)

        @pl.when(g > 0)
        def _():
            sum_first(g - 1)

        @pl.when(g > 1)
        def _():
            norm_first(g - 2)

        lax.fori_loop(0, pieces, seen_of, 0)
        send_first(g)
        return carry

    lax.fori_loop(0, groups, group, 0)
    passes = [
        (0, rows - CHUNK, own2, term2, rs2, yb, 0),
        (rows - CHUNK, CHUNK, own3, term3, rs3, yc, 1),
    ]
    ff = wg_v.shape[1]
    block = ff // 2

    def gate(p):
        lo, tall = passes[p][:2]

        def body(i, carry):
            at = pl.ds(pl.multiple_of(i * block, block), block)
            gates[lo : lo + tall, at] = dot(act[lo : lo + tall, :], wg_v[:, at])
            return carry

        lax.fori_loop(0, ff // block, body, 0)

    def up(p):
        lo, tall = passes[p][:2]

        def body(i, carry):
            at = pl.ds(pl.multiple_of(i * block, block), block)
            u = dot(act[lo : lo + tall, :], wu_v[:, at])
            hidden[lo : lo + tall, at] = (jax.nn.silu(gates[lo : lo + tall, at]) * u).astype(BF16)
            return carry

        lax.fori_loop(0, ff // block, body, 0)

    def both(p):
        lo, tall = passes[p][:2]
        for i in range(0, ff, block):
            g = dot(act[lo : lo + tall, :], wg_v[:, i : i + block])
            u = dot(act[lo : lo + tall, :], wu_v[:, i : i + block])
            hidden[lo : lo + tall, i : i + block] = (jax.nn.silu(g) * u).astype(BF16)

    def down(p):
        lo, tall, own, term, land, _, k = passes[p]
        tall1 = tall // (n // across)

        def body(i, carry):
            at = lax.rem(me + i, across // 2)
            res = dot(hidden[lo : lo + tall, :], wd_v[:, pl.ds(pl.multiple_of(at * 2 * wide1, 2 * wide1), 2 * wide1)])
            for cg in range(2):
                for rg in range(n // across):
                    to = rg * across + at * 2 + cg
                    part = res[rg * tall1 : (rg + 1) * tall1, cg * wide1 : (cg + 1) * wide1]
                    own[to] = part
                    term[to] = part.astype(BF16)

                    @pl.when(to != me)
                    def _():
                        send_to(to, term.at[to], land.at[lax.rem(to - me + n, n) - 1], send3.at[k], recv3.at[k])

            return carry

        lax.fori_loop(0, across // 2, body, 0)

    norm_first(chunks - 2)
    weights[0].wait()
    gate(0)
    sum_first(chunks - 1)
    weights[1].wait()
    up(0)
    weights[2].wait()
    down(0)
    norm_first(chunks - 1)
    both(1)
    down(1)
    for lo, tall, own, term, land, buf, k in passes:
        finish(h32, lo, own, land, buf, recv3.at[k], send4.at[k], recv4.at[k])
    for lo, tall, own, term, land, buf, k in passes:
        total(buf, recv4.at[k])
        out_ref[lo : lo + tall, :] = whole(buf).astype(BF16)
    for c in range(chunks):
        total(term1.at[c], send1.at[c])
        total(hb.at[c], send2.at[c])
    for lo, tall, own, term, land, buf, k in passes:
        total(term, send3.at[k])
        total(buf, send4.at[k])


def solution(mesh):
    n = mesh.shape["tp"]

    def step(x, k_cache, v_cache, gain_a, wq, wo, gain_m, w_gate, w_up, w_down):
        rows, d = x.shape
        cache = k_cache.shape[1]
        head = k_cache.shape[3]
        ff = w_gate.shape[1]
        half = head // 2
        angle = (cache - 1) * float(THETA) ** (-np.arange(half, dtype=np.float64) / half)
        trig = jnp.asarray(np.stack([np.cos(angle), np.sin(angle)]).astype(np.float32))
        chunks = rows // CHUNK
        share = (SUB, rows * d // chunks // n // SUB)
        any_spec = pl.BlockSpec(memory_space=pl.ANY)
        dma = pltpu.SemaphoreType.DMA
        call = pl.pallas_call(
            functools.partial(kernel, n),
            out_shape=jax.ShapeDtypeStruct((rows, d), BF16),
            in_specs=[any_spec] * 11,
            out_specs=pl.BlockSpec(memory_space=pltpu.VMEM),
            scratch_shapes=[
                pltpu.VMEM((rows, d), BF16),
                pltpu.VMEM((d,), BF16),
                pltpu.VMEM((d,), BF16),
                pltpu.VMEM((2, half), F32),
                pltpu.VMEM((d, head), BF16),
                pltpu.VMEM((head, d), BF16),
                pltpu.VMEM((d, ff), BF16),
                pltpu.VMEM((d, ff), BF16),
                pltpu.VMEM((ff, d), BF16),
                pltpu.VMEM((GROUP // PIECE, PIECE, cache, head), BF16),
                pltpu.VMEM((rows, d), F32),
                pltpu.VMEM((rows, d), F32),
                pltpu.VMEM((rows, head), F32),
                pltpu.VMEM((rows, head), F32),
                pltpu.VMEM((GROUP, cache), F32),
                pltpu.VMEM((rows, d), BF16),
                pltpu.VMEM((rows, ff), BF16),
                pltpu.VMEM((rows, ff), F32),
                pltpu.VMEM((chunks, n, *share), F32),
                pltpu.VMEM((chunks, n, *share), BF16),
                pltpu.VMEM((chunks, n - 1, *share), BF16),
                pltpu.VMEM((chunks, n, *share), BF16),
            ]
            + [
                pltpu.VMEM((m, t, share[1]), kind)
                for t in (SUB * (chunks - 1), SUB)
                for m, kind in ((n, F32), (n, BF16), (n - 1, BF16), (n, BF16))
            ]
            + [
                dma((6,)),
                dma((3,)),
                dma((GROUP // PIECE,)),
            ]
            + [dma((chunks,))] * 4
            + [dma((2,))] * 4,
            compiler_params=pltpu.CompilerParams(collective_id=0, has_side_effects=True, vmem_limit_bytes=63 * 2**20),
        )
        flat = (rows, cache, head)
        return call(
            x, k_cache.reshape(flat), v_cache.reshape(flat), gain_a, wq, wo, gain_m, w_gate, w_up, w_down, trig
        )

    states, cache, columns, rows_of = P("dp", None), P("dp", None, "tp", None), P(None, "tp"), P("tp", None)
    return jax.shard_map(
        step,
        mesh=mesh,
        in_specs=(states, cache, cache, P(None), columns, rows_of, P(None), columns, columns, rows_of),
        out_specs=states,
        check_vma=False,
    )
```

```python
import functools

import jax
import jax.numpy as jnp
import numpy as np
from jax import lax
from jax.experimental import pallas as pl
from jax.experimental.pallas import tpu as pltpu
from jax.sharding import PartitionSpec as P

THETA = 10000
EPS = 1e-6
GROUP = 16
PIECE = 4
CHUNK = 16
SUB = 8
MESH = pl.DeviceIdType.MESH
BF16, F32 = jnp.bfloat16, jnp.float32


def normed(wide, gain):
    scale = lax.rsqrt(jnp.mean(wide * wide, -1, keepdims=True) + EPS)
    return (wide * scale * gain).astype(BF16)


def dot(a, b):
    return jnp.dot(a, b, preferred_element_type=F32)


def kernel(n, x_hbm, k_hbm, v_hbm, ga_hbm, wq_hbm, wo_hbm, gm_hbm, wg_hbm, wu_hbm, wd_hbm, trig_hbm, out_ref,
           x_v, ga_v, gm_v, trig_v, wq_v, wo_v, wg_v, wu_v, wd_v, ring, x32, h32, q32, seen32, scores, act, hidden,
           gates, own1, term1, rs1, hb, own2, term2, rs2, yb, own3, term3, rs3, yc,
           in_sem, w_sem, ring_sem, send1, recv1, send2, recv2, send3, recv3, send4, recv4):
    me = lax.axis_index("tp")
    rows, d = x_v.shape
    head = q32.shape[1]
    half = head // 2
    groups = rows // GROUP
    chunks = rows // CHUNK
    across = n * SUB // CHUNK
    wide1 = d // across

    def fetch(src, dst, sem):
        return pltpu.make_async_copy(src, dst, sem)

    small = [
        fetch(x_hbm, x_v, in_sem.at[0]),
        fetch(ga_hbm, ga_v, in_sem.at[1]),
        fetch(wq_hbm, wq_v, in_sem.at[2]),
        fetch(trig_hbm, trig_v, in_sem.at[3]),
        fetch(wo_hbm, wo_v, in_sem.at[4]),
        fetch(gm_hbm, gm_v, in_sem.at[5]),
    ]
    weights = [fetch(wg_hbm, wg_v, w_sem.at[0]), fetch(wu_hbm, wu_v, w_sem.at[1]), fetch(wd_hbm, wd_v, w_sem.at[2])]

    def piece(src, g, j):
        return fetch(src.at[pl.ds(g * GROUP + j * PIECE, PIECE)], ring.at[j], ring_sem.at[j])

    for c in small[:4]:
        c.start()
    for j in range(GROUP // PIECE):
        piece(k_hbm, 0, j).start()
    for c in small[4:]:
        c.start()

    barrier = pltpu.get_barrier_semaphore()
    for r in range(1, n):
        pl.semaphore_signal(barrier, inc=1, device_id={"tp": lax.rem(me + r, n)}, device_id_type=MESH)

    small[0].wait()
    small[1].wait()
    wide = x_v[...].astype(F32)
    x32[...] = wide
    act[...] = normed(wide, ga_v[...].astype(F32).reshape(1, d))
    small[2].wait()
    small[3].wait()
    q = dot(act[...], wq_v[...]).astype(BF16).astype(F32)
    cos, sin = trig_v[0:1, :], trig_v[1:2, :]
    a, b = q[:, :half], q[:, half:]
    q32[:, :half] = (a * cos - b * sin).astype(BF16).astype(F32)
    q32[:, half:] = (b * cos + a * sin).astype(BF16).astype(F32)
    small[4].wait()
    small[5].wait()
    pl.semaphore_wait(barrier, n - 1)

    def total(buf, sem):
        fetch(buf.at[pl.ds(0, n - 1)], buf.at[pl.ds(0, n - 1)], sem).wait()

    def send_to(to, src, dst, send, recv):
        pltpu.make_async_remote_copy(
            src_ref=src, dst_ref=dst, send_sem=send, recv_sem=recv, device_id={"tp": to}, device_id_type=MESH
        ).start()

    def gather(buf, send, recv):
        for r in range(1, n):
            send_to(lax.rem(me + r, n), buf.at[me], buf.at[me], send, recv)

    def share_of(states, row, buf):
        tall, wide = buf.shape[1:]
        row = pl.multiple_of(row + me // across * tall, SUB)
        return states[pl.ds(row, tall), pl.ds(pl.multiple_of(lax.rem(me, across) * wide, 128), wide)]

    def finish(states, row, own, land, buf, recv, send_next, recv_next):
        total(land, recv)
        s = own[me]
        for r in range(n - 1):
            s = s + land[r].astype(F32)
        buf[me] = (share_of(states, row, buf) + s).astype(BF16)
        gather(buf, send_next, recv_next)

    def whole(buf):
        rows_of = [jnp.concatenate([buf[rg * across + cg].astype(F32) for cg in range(across)], 1) for rg in range(n // across)]
        return jnp.concatenate(rows_of, 0)

    def send_first(c):
        res = dot(seen32[pl.ds(pl.multiple_of(c * CHUNK, CHUNK), CHUNK), :].astype(BF16), wo_v[...])
        for to in range(n):
            rg, cg = divmod(to, across)
            part = res[rg * SUB : (rg + 1) * SUB, cg * wide1 : (cg + 1) * wide1]
            own1[c, to] = part
            term1[c, to] = part.astype(BF16)
        for r in range(1, n):
            to = lax.rem(me + r, n)
            send_to(to, term1.at[c, to], rs1.at[c, r - 1], send1.at[c], recv1.at[c])

    def sum_first(c):
        finish(x32, c * CHUNK, own1.at[c], rs1.at[c], hb.at[c], recv1.at[c], send2.at[c], recv2.at[c])

    def norm_first(c):
        total(hb.at[c], recv2.at[c])
        h = whole(hb.at[c])
        at = pl.ds(pl.multiple_of(c * CHUNK, CHUNK), CHUNK)
        h32[at, :] = h
        act[at, :] = normed(h, gm_v[...].astype(F32).reshape(1, d))

    row_of = lax.broadcasted_iota(jnp.int32, (GROUP, 1), 0)
    pieces = GROUP // PIECE

    def group(g, carry):
        at = pl.ds(pl.multiple_of(g * GROUP, GROUP), GROUP)

        def scores_of(j, carry):
            qg = q32[at, :]
            piece(k_hbm, g, j).wait()
            s = None
            for i in range(PIECE):
                qm = jnp.where(row_of == j * PIECE + i, qg, 0.0).astype(BF16)
                t = lax.dot_general(qm, ring[j, i], (((1,), (1,)), ((), ())), preferred_element_type=F32)
                s = t if s is None else s + t
            scores[...] = jnp.where(row_of // PIECE == j, s, scores[...])
            piece(v_hbm, g, j).start()
            return carry

        def seen_of(j, carry):
            piece(v_hbm, g, j).wait()
            o = []
            for i in range(PIECE):
                wm = jnp.where(row_of == j * PIECE + i, scores[...], 0.0).astype(BF16)
                o.append(dot(wm, ring[j, i]))
            o = jnp.where(row_of < j * PIECE + PIECE // 2, sum(o[1 : PIECE // 2], o[0]), sum(o[PIECE // 2 + 1 :], o[PIECE // 2]))
            seen32[at, :] = jnp.where(row_of // PIECE == j, o, seen32[at, :])

            @pl.when(g < groups - 1)
            def _():
                piece(k_hbm, g + 1, j).start()

            for w in range(3):
                @pl.when(jnp.logical_and(g == groups - 1, j == w))
                def _():
                    weights[w].start()

            return carry

        lax.fori_loop(0, pieces, scores_of, 0)
        s = scores[...] * head**-0.5
        p = jnp.exp(s - jnp.max(s, -1, keepdims=True))
        scores[...] = p / jnp.sum(p, -1, keepdims=True)

        @pl.when(g > 0)
        def _():
            sum_first(g - 1)

        @pl.when(g > 1)
        def _():
            norm_first(g - 2)

        lax.fori_loop(0, pieces, seen_of, 0)
        send_first(g)
        return carry

    lax.fori_loop(0, groups, group, 0)
    passes = [
        (0, rows - CHUNK, own2, term2, rs2, yb, 0),
        (rows - CHUNK, CHUNK, own3, term3, rs3, yc, 1),
    ]
    ff = wg_v.shape[1]
    block = ff // 2

    def gate(p):
        lo, tall = passes[p][:2]

        def body(i, carry):
            at = pl.ds(pl.multiple_of(i * block, block), block)
            gates[lo : lo + tall, at] = dot(act[lo : lo + tall, :], wg_v[:, at])
            return carry

        lax.fori_loop(0, ff // block, body, 0)

    def up(p):
        lo, tall = passes[p][:2]

        def body(i, carry):
            at = pl.ds(pl.multiple_of(i * block, block), block)
            u = dot(act[lo : lo + tall, :], wu_v[:, at])
            hidden[lo : lo + tall, at] = (jax.nn.silu(gates[lo : lo + tall, at]) * u).astype(BF16)
            return carry

        lax.fori_loop(0, ff // block, body, 0)

    def both(p):
        lo, tall = passes[p][:2]
        for i in range(0, ff, block):
            g = dot(act[lo : lo + tall, :], wg_v[:, i : i + block])
            u = dot(act[lo : lo + tall, :], wu_v[:, i : i + block])
            hidden[lo : lo + tall, i : i + block] = (jax.nn.silu(g) * u).astype(BF16)

    def down(p):
        lo, tall, own, term, land, _, k = passes[p]
        tall1 = tall // (n // across)

        def body(i, carry):
            at = lax.rem(me + i, across // 2)
            res = dot(hidden[lo : lo + tall, :], wd_v[:, pl.ds(pl.multiple_of(at * 2 * wide1, 2 * wide1), 2 * wide1)])
            for cg in range(2):
                for rg in range(n // across):
                    to = rg * across + at * 2 + cg
                    part = res[rg * tall1 : (rg + 1) * tall1, cg * wide1 : (cg + 1) * wide1]
                    own[to] = part
                    term[to] = part.astype(BF16)

                    @pl.when(to != me)
                    def _():
                        send_to(to, term.at[to], land.at[lax.rem(to - me + n, n) - 1], send3.at[k], recv3.at[k])

            return carry

        lax.fori_loop(0, across // 2, body, 0)

    norm_first(chunks - 2)
    weights[0].wait()
    gate(0)
    sum_first(chunks - 1)
    weights[1].wait()
    up(0)
    weights[2].wait()
    down(0)
    norm_first(chunks - 1)
    both(1)
    down(1)
    for lo, tall, own, term, land, buf, k in passes:
        finish(h32, lo, own, land, buf, recv3.at[k], send4.at[k], recv4.at[k])
    for lo, tall, own, term, land, buf, k in passes:
        total(buf, recv4.at[k])
        out_ref[lo : lo + tall, :] = whole(buf).astype(BF16)
    for c in range(chunks):
        total(term1.at[c], send1.at[c])
        total(hb.at[c], send2.at[c])
    for lo, tall, own, term, land, buf, k in passes:
        total(term, send3.at[k])
        total(buf, send4.at[k])


def solution(mesh):
    n = mesh.shape["tp"]

    def step(x, k_cache, v_cache, gain_a, wq, wo, gain_m, w_gate, w_up, w_down):
        rows, d = x.shape
        cache = k_cache.shape[1]
        head = k_cache.shape[3]
        ff = w_gate.shape[1]
        half = head // 2
        angle = (cache - 1) * float(THETA) ** (-np.arange(half, dtype=np.float64) / half)
        trig = jnp.asarray(np.stack([np.cos(angle), np.sin(angle)]).astype(np.float32))
        chunks = rows // CHUNK
        share = (SUB, rows * d // chunks // n // SUB)
        any_spec = pl.BlockSpec(memory_space=pltpu.HBM)
        dma = pltpu.SemaphoreType.DMA
        call = pl.pallas_call(
            functools.partial(kernel, n),
            out_shape=pltpu.VMEM((rows, d), BF16),
            in_specs=[any_spec] * 11,
            out_specs=pl.BlockSpec(memory_space=pltpu.VMEM),
            scratch_shapes=[
                pltpu.VMEM((rows, d), BF16),
                pltpu.VMEM((d,), BF16),
                pltpu.VMEM((d,), BF16),
                pltpu.VMEM((2, half), F32),
                pltpu.VMEM((d, head), BF16),
                pltpu.VMEM((head, d), BF16),
                pltpu.VMEM((d, ff), BF16),
                pltpu.VMEM((d, ff), BF16),
                pltpu.VMEM((ff, d), BF16),
                pltpu.VMEM((GROUP // PIECE, PIECE, cache, head), BF16),
                pltpu.VMEM((rows, d), F32),
                pltpu.VMEM((rows, d), F32),
                pltpu.VMEM((rows, head), F32),
                pltpu.VMEM((rows, head), F32),
                pltpu.VMEM((GROUP, cache), F32),
                pltpu.VMEM((rows, d), BF16),
                pltpu.VMEM((rows, ff), BF16),
                pltpu.VMEM((rows, ff), F32),
                pltpu.VMEM((chunks, n, *share), F32),
                pltpu.VMEM((chunks, n, *share), BF16),
                pltpu.VMEM((chunks, n - 1, *share), BF16),
                pltpu.VMEM((chunks, n, *share), BF16),
            ]
            + [
                pltpu.VMEM((m, t, share[1]), kind)
                for t in (SUB * (chunks - 1), SUB)
                for m, kind in ((n, F32), (n, BF16), (n - 1, BF16), (n, BF16))
            ]
            + [
                dma((6,)),
                dma((3,)),
                dma((GROUP // PIECE,)),
            ]
            + [dma((chunks,))] * 4
            + [dma((2,))] * 4,
            compiler_params=pltpu.CompilerParams(collective_id=0, has_side_effects=True, vmem_limit_bytes=58 * 2**20),
        )
        flat = (rows, cache, head)
        return call(
            x, k_cache.reshape(flat), v_cache.reshape(flat), gain_a, wq, wo, gain_m, w_gate, w_up, w_down, trig
        )

    states, cache, columns, rows_of = P("dp", None), P("dp", None, "tp", None), P(None, "tp"), P("tp", None)
    return jax.shard_map(
        step,
        mesh=mesh,
        in_specs=(states, cache, cache, P(None), columns, rows_of, P(None), columns, columns, rows_of),
        out_specs=states,
        check_vma=False,
    )
```
